8 devices in a mesh: replica: 2 (over z, y), seq: 4 (over x, core).
Axes of the slice: x: 2, y: 2, z: 1, core: 2. Of those that a mesh axis runs over, the one named last changes fastest.
Arguments:
- query_in: bfloat16 [8, 256, 3072], P('replica', 'seq'), parts along dimension 0
- memory: bfloat16 [8, 2048, 3072], P('replica', 'seq'), parts along dimension 0
- mem_len: int32 [8], P('replica'), parts along dimension 0
- w_query: bfloat16 [3072, 16, 256], replicated
- w_key: bfloat16 [3072, 16, 256], replicated
- w_value: bfloat16 [3072, 16, 256], replicated
- w_out: bfloat16 [16, 256, 3072], replicated
Outputs:
- output: bfloat16 [8, 256, 3072], P('replica', 'seq'), parts along dimension 0
There are 2 independent parts. The reference program is written for one: setup_inputs(seed, part) draws one part's arguments, and reference() takes and returns one part's arrays. A program takes and returns all parts, laid end to end along the dimension named above; an argument that names none is the same for every part.
All inputs are finite; a program needn't handle non-finite values.
Results may differ from the reference program's by a relative error of at most 0.00767016.
Values are sent between devices in bfloat16 or wider.
A program may use at most 1 GiB of HBM per device.

```python
import math
import jax
import jax.numpy as jnp
from jax import lax

BATCH_SIZE = 4
NUM_QUERIES = 256
MEM_LEN = 2048
MODEL_DIM = 3072
NUM_HEADS = 16
KV_HEADS = 16
HEAD_DIM = 256
GROUP_SIZE = NUM_HEADS // KV_HEADS
MEM_BLOCK = math.gcd(MEM_LEN, 256)
NUM_BLOCKS = MEM_LEN // MEM_BLOCK
NEG_BIG = -1e30


def setup_inputs(seed: int = 0, part: int = 0) -> dict:
    part_keys = jax.random.split(jax.random.fold_in(jax.random.key(seed), part), 4)
    weight_keys = jax.random.split(jax.random.key(seed + 1), 4)
    query_in = jax.random.normal(part_keys[0], (BATCH_SIZE, NUM_QUERIES, MODEL_DIM), jnp.float32)
    memory = jax.random.normal(part_keys[1], (BATCH_SIZE, MEM_LEN, MODEL_DIM), jnp.float32)
    lengths = jax.random.randint(part_keys[2], (BATCH_SIZE,), MEM_LEN // 4, MEM_LEN + 1)
    full_row = jax.random.randint(part_keys[3], (), 0, BATCH_SIZE)
    mem_len = jnp.where(jnp.arange(BATCH_SIZE) == full_row, MEM_LEN, lengths).astype(jnp.int32)
    in_scale = MODEL_DIM ** -0.5
    out_scale = 0.1 * math.sqrt(MEM_LEN / (NUM_HEADS * HEAD_DIM))
    w_query = 2.0 * in_scale * jax.random.normal(weight_keys[0], (MODEL_DIM, NUM_HEADS, HEAD_DIM), jnp.float32)
    w_key = in_scale * jax.random.normal(weight_keys[1], (MODEL_DIM, KV_HEADS, HEAD_DIM), jnp.float32)
    w_value = in_scale * jax.random.normal(weight_keys[2], (MODEL_DIM, KV_HEADS, HEAD_DIM), jnp.float32)
    w_out = out_scale * jax.random.normal(weight_keys[3], (NUM_HEADS, HEAD_DIM, MODEL_DIM), jnp.float32)
    return {
        'query_in': query_in.astype(jnp.bfloat16),
        'memory': memory.astype(jnp.bfloat16),
        'mem_len': mem_len,
        'w_query': w_query.astype(jnp.bfloat16),
        'w_key': w_key.astype(jnp.bfloat16),
        'w_value': w_value.astype(jnp.bfloat16),
        'w_out': w_out.astype(jnp.bfloat16),
    }


def reference(query_in, memory, mem_len, w_query, w_key, w_value, w_out):
    score_scale = 1.0 / math.sqrt(HEAD_DIM)
    queries = jnp.dot(query_in.reshape(BATCH_SIZE * NUM_QUERIES, MODEL_DIM), w_query.reshape(MODEL_DIM, NUM_HEADS * HEAD_DIM), preferred_element_type=jnp.float32).astype(jnp.bfloat16)
    queries = queries.reshape(BATCH_SIZE, NUM_QUERIES, KV_HEADS, GROUP_SIZE, HEAD_DIM).astype(jnp.float32)
    key_mat = w_key.reshape(MODEL_DIM, KV_HEADS * HEAD_DIM)
    value_mat = w_value.reshape(MODEL_DIM, KV_HEADS * HEAD_DIM)

    def scan_step(carry, blk_start):
        run_max, run_sum, run_out = carry
        mem_blk = lax.dynamic_slice_in_dim(memory, blk_start, MEM_BLOCK, axis=1).reshape(BATCH_SIZE * MEM_BLOCK, MODEL_DIM)
        key_blk = jnp.dot(mem_blk, key_mat, preferred_element_type=jnp.float32).astype(jnp.bfloat16)
        key_blk = key_blk.reshape(BATCH_SIZE, MEM_BLOCK, KV_HEADS, HEAD_DIM).astype(jnp.float32)
        val_blk = jnp.dot(mem_blk, value_mat, preferred_element_type=jnp.float32).astype(jnp.bfloat16)
        val_blk = val_blk.reshape(BATCH_SIZE, MEM_BLOCK, KV_HEADS, HEAD_DIM).astype(jnp.float32)
        scores = jnp.einsum('bqkgd,btkd->bkqgt', queries, key_blk) * score_scale
        position = blk_start + jnp.arange(MEM_BLOCK)
        is_valid = position[None, :] < mem_len[:, None]
        scores = jnp.where(is_valid[:, None, None, None, :], scores, NEG_BIG)
        new_max = jnp.maximum(run_max, jnp.max(scores, axis=-1))
        weights = jnp.exp(scores - new_max[..., None])
        factor = jnp.exp(run_max - new_max)
        new_sum = run_sum * factor + jnp.sum(weights, axis=-1)
        weights_low = weights.astype(jnp.bfloat16).astype(jnp.float32)
        new_out = run_out * factor[..., None] + jnp.einsum('bkqgt,btkd->bkqgd', weights_low, val_blk)
        return (new_max, new_sum, new_out), None

    stat_shape = (BATCH_SIZE, KV_HEADS, NUM_QUERIES, GROUP_SIZE)
    init_carry = (jnp.full(stat_shape, NEG_BIG, jnp.float32), jnp.zeros(stat_shape, jnp.float32), jnp.zeros(stat_shape + (HEAD_DIM,), jnp.float32))
    block_starts = jnp.arange(NUM_BLOCKS) * MEM_BLOCK
    final_carry, _ = lax.scan(scan_step, init_carry, block_starts)
    run_sum = final_carry[1]
    run_out = final_carry[2]
    attended = (run_out / run_sum[..., None]).astype(jnp.bfloat16)
    attended = attended.transpose(0, 2, 1, 3, 4).reshape(BATCH_SIZE * NUM_QUERIES, NUM_HEADS * HEAD_DIM)
    result = jnp.dot(attended, w_out.reshape(NUM_HEADS * HEAD_DIM, MODEL_DIM), preferred_element_type=jnp.float32).astype(jnp.bfloat16)
    return result.reshape(BATCH_SIZE, NUM_QUERIES, MODEL_DIM)
```

```python
import functools
import math
import jax
import jax.numpy as jnp
from jax import lax
from jax.experimental import pallas as pl
from jax.experimental.pallas import tpu as pltpu
from jax.sharding import PartitionSpec as P

NEG_BIG = -1e30
BF16 = jnp.bfloat16
F32 = jnp.float32


def attend_kernel(len_ref, qin_hbm, mem_hbm, wq_hbm, wk_hbm, wv_hbm,
                  oown_hbm, sown_hbm, orecv_hbm, srecv_hbm,
                  x_buf, q_in, q_all, raw_k, raw_v, w_a, w_b, kv, o_send, o_own, s_send, s_own,
                  x_sem, xr_send, xr_recv, qi_sem, qi_send, qi_recv, raw_sem,
                  q_send, q_recv, o_ssem, o_rsem, s_ssem, s_rsem, oo_sem, so_sem):
    me = lax.axis_index('seq')
    chip = me // 2
    core = lax.rem(me, 2)
    partner = 2 * chip + (1 - core)
    cross = 2 * (1 - chip) + core
    n_batch = mem_hbm.shape[0]
    d_model = mem_hbm.shape[2]
    head_dim = wq_hbm.shape[2]
    n_heads = wq_hbm.shape[1] // 2
    n_pairs = n_heads // 2
    head0 = core * n_heads
    rows = mem_hbm.shape[1]
    half_q = q_all.shape[2] // n_batch
    scale = 1.0 / math.sqrt(head_dim)

    def to(dev):
        return dict(device_id={'seq': dev}, device_id_type=pl.DeviceIdType.MESH)

    def raw_copy(src, dst, pair, sem):
        return pltpu.make_async_copy(src.at[:, pl.ds(head0 + 2 * pair, 2), :], dst, sem)

    x_local = [pltpu.make_async_copy(mem_hbm.at[b], x_buf.at[2 * b + core], x_sem.at[b]) for b in range(n_batch)]
    qi_local = pltpu.make_async_copy(qin_hbm, q_in.at[:, core], qi_sem)
    qi_local.start()
    raw_copy(wq_hbm, raw_k, 0, raw_sem.at[0]).start()
    raw_copy(wq_hbm, raw_v, 1, raw_sem.at[1]).start()
    for c in x_local:
        c.start()

    barrier = pltpu.get_barrier_semaphore()
    pl.semaphore_signal(barrier, inc=1, **to(partner))
    pl.semaphore_signal(barrier, inc=1, **to(cross))
    pl.semaphore_wait(barrier, 2)

    qi_remote = pltpu.make_async_remote_copy(qin_hbm, q_in.at[:, core], qi_send, qi_recv, **to(partner))
    qi_remote.start()
    x_remote = [pltpu.make_async_remote_copy(mem_hbm.at[b], x_buf.at[2 * b + core], xr_send.at[b], xr_recv.at[b], **to(partner)) for b in range(n_batch)]
    for c in x_remote:
        c.start()

    chunk = 384
    n_chunks = d_model // chunk

    def relayout(raw, dst, lane, i):
        r = pl.ds(pl.multiple_of(i * chunk, chunk), chunk)
        dst[:, r, lane:lane + head_dim] = jnp.swapaxes(raw[r], 0, 1)

    qi_local.wait()
    qi_remote.wait()
    for pair in range(n_pairs):
        raw = raw_k if pair % 2 == 0 else raw_v
        raw_copy(wq_hbm, raw, pair, raw_sem.at[pair % 2]).wait()

        def q_chunk(i, carry, raw=raw):
            relayout(raw, w_b, 0, i)
            return carry

        lax.fori_loop(0, n_chunks, q_chunk, 0)
        if pair + 2 < n_pairs:
            raw_copy(wq_hbm, raw, pair + 2, raw_sem.at[pair % 2]).start()
        elif pair % 2 == 0:
            raw_copy(wk_hbm, raw_k, 0, raw_sem.at[0]).start()
        else:
            raw_copy(wv_hbm, raw_v, 0, raw_sem.at[1]).start()
        for j in range(2):
            def q_dot(b, carry, j=j, pair=pair):
                q_rows = q_in[pl.ds(2 * b, 2)].reshape(4 * q_in.shape[2], d_model)
                n = q_rows.shape[0]
                res = jnp.dot(q_rows, w_b[j, :, 0:head_dim], preferred_element_type=F32)
                q_all[0, 2 * pair + j, pl.ds(pl.multiple_of(b * n, n), n), :] = res.astype(BF16)
                return carry

            lax.fori_loop(0, n_batch // 2, q_dot, 0)
        sl = pl.ds(2 * pair, 2)
        pltpu.make_async_remote_copy(q_all.at[0, sl], q_all.at[1, sl], q_send.at[pair], q_recv.at[pair], **to(cross)).start()

    raw_copy(wk_hbm, raw_k, 0, raw_sem.at[0]).wait()
    raw_copy(wv_hbm, raw_v, 0, raw_sem.at[1]).wait()

    def first(i, carry):
        relayout(raw_k, w_a, 0, i)
        relayout(raw_v, w_a, head_dim, i)
        return carry

    lax.fori_loop(0, n_chunks, first, 0)
    raw_copy(wk_hbm, raw_k, 1, raw_sem.at[0]).start()
    raw_copy(wv_hbm, raw_v, 1, raw_sem.at[1]).start()

    for head in range(n_heads):
        pair, j = head // 2, head % 2
        w_now, w_next = (w_a, w_b) if pair % 2 == 0 else (w_b, w_a)
        prep = j == 1 and pair + 1 < n_pairs
        if prep:
            raw_copy(wk_hbm, raw_k, pair + 1, raw_sem.at[0]).wait()
            raw_copy(wv_hbm, raw_v, pair + 1, raw_sem.at[1]).wait()

        def kv_tile(t, carry, own, w_now=w_now, w_next=w_next, j=j, prep=prep):
            slot = 2 * t + (core if own else 1 - core)
            if prep:
                i = t if own else t + n_batch
                relayout(raw_k, w_next, 0, i)
                relayout(raw_v, w_next, head_dim, i)
            res = jnp.dot(x_buf[slot], w_now[j], preferred_element_type=F32)
            kv[slot] = res.astype(BF16)
            return carry

        if head == 0:
            for c in x_local:
                c.wait()
        lax.fori_loop(0, n_batch, functools.partial(kv_tile, own=True), 0)
        if head == 0:
            for c in x_remote:
                c.wait()
        lax.fori_loop(0, n_batch, functools.partial(kv_tile, own=False), 0)
        if prep and pair + 2 < n_pairs:
            raw_copy(wk_hbm, raw_k, pair + 2, raw_sem.at[0]).start()
            raw_copy(wv_hbm, raw_v, pair + 2, raw_sem.at[1]).start()
        sl = pl.ds(2 * pair, 2)
        if j == 0:
            pltpu.make_async_remote_copy(q_all.at[0, sl], q_all.at[1, sl], q_send.at[pair], q_recv.at[pair], **to(cross)).wait()

        slot = head % 2

        def sends(h):
            k = h % 2
            return (
                pltpu.make_async_remote_copy(o_send.at[k], orecv_hbm.at[h], o_ssem.at[k], o_rsem.at[h], **to(cross)),
                pltpu.make_async_remote_copy(s_send.at[k], srecv_hbm.at[h], s_ssem.at[k], s_rsem.at[h], **to(cross)),
                pltpu.make_async_copy(o_own.at[k], oown_hbm.at[h], oo_sem.at[k]),
                pltpu.make_async_copy(s_own.at[k], sown_hbm.at[h], so_sem.at[k]),
            )

        if head >= 2:
            a, b_, c_, d_ = sends(head - 2)
            a.wait_send()
            b_.wait_send()
            c_.wait()
            d_.wait()

        for b in range(n_batch):
            q_sl = pl.ds(b * half_q, half_q)
            q = jnp.concatenate([q_all[0, head, q_sl, :], q_all[1, head, q_sl, :]], axis=0)
            k_b = kv[2 * b:2 * b + 2, :, 0:head_dim].reshape(2 * rows, head_dim)
            v_b = kv[2 * b:2 * b + 2, :, head_dim:].reshape(2 * rows, head_dim)
            s = lax.dot_general(q, k_b, (((1,), (1,)), ((), ())), preferred_element_type=F32) * scale
            pos = lax.broadcasted_iota(jnp.int32, s.shape, 1)
            s = jnp.where(pos < len_ref[b] - chip * (2 * rows), s, NEG_BIG)
            m = jnp.max(s, axis=1, keepdims=True)
            p = jnp.exp(s - m)
            l = jnp.sum(p, axis=1, keepdims=True)
            o = jnp.dot(p.astype(BF16), v_b, preferred_element_type=F32)
            o_own[slot, q_sl, :] = o[:half_q]
            o_send[slot, q_sl, :] = o[half_q:]
            lane = lax.broadcasted_iota(jnp.int32, (2 * half_q, 128), 1)
            stat = jnp.where(lane == 0, m, l).T[0:8]
            s_own[slot, :, b * half_q:(b + 1) * half_q] = stat[:, :half_q]
            s_send[slot, :, b * half_q:(b + 1) * half_q] = stat[:, half_q:]
        for c in sends(head):
            c.start()

    for h in range(n_heads):
        a, b_, c_, d_ = sends(h)
        a.wait_recv()
        b_.wait_recv()
        if h >= n_heads - 2:
            a.wait_send()
            b_.wait_send()
            c_.wait()
            d_.wait()


def attend(mem_len, query_in, memory, w_query, w_key, w_value):
    n_batch, q_loc, d_model = query_in.shape
    mem_local = memory.shape[1]
    head_dim = w_query.shape[2]
    n_heads = w_query.shape[1] // 2
    n_pairs = n_heads // 2
    n_rows = n_batch * 2 * q_loc
    any_spec = pl.BlockSpec(memory_space=pl.ANY)
    part = jax.ShapeDtypeStruct((n_heads, n_rows, head_dim), F32)
    stat = jax.ShapeDtypeStruct((n_heads, 8, n_rows), F32)
    dma = pltpu.SemaphoreType.DMA
    return pl.pallas_call(
        attend_kernel,
        out_shape=(part, stat, part, stat),
        in_specs=[pl.BlockSpec(memory_space=pltpu.SMEM)] + [any_spec] * 5,
        out_specs=(any_spec,) * 4,
        scratch_shapes=[
            pltpu.VMEM((2 * n_batch, mem_local, d_model), BF16),
            pltpu.VMEM((n_batch, 2, q_loc, d_model), BF16),
            pltpu.VMEM((2, n_heads, n_rows, head_dim), BF16),
            pltpu.VMEM((d_model, 2, head_dim), BF16),
            pltpu.VMEM((d_model, 2, head_dim), BF16),
            pltpu.VMEM((2, d_model, 2 * head_dim), BF16),
            pltpu.VMEM((2, d_model, 2 * head_dim), BF16),
            pltpu.VMEM((2 * n_batch, mem_local, 2 * head_dim), BF16),
            pltpu.VMEM((2, n_rows, head_dim), F32),
            pltpu.VMEM((2, n_rows, head_dim), F32),
            pltpu.VMEM((2, 8, n_rows), F32),
            pltpu.VMEM((2, 8, n_rows), F32),
            dma((n_batch,)), dma((n_batch,)), dma((n_batch,)), dma, dma, dma, dma((2,)),
            dma((n_pairs,)), dma((n_pairs,)), dma((2,)), dma((n_heads,)), dma((2,)), dma((n_heads,)), dma((2,)), dma((2,)),
        ],
        compiler_params=pltpu.CompilerParams(collective_id=0, has_side_effects=True, vmem_limit_bytes=67043328),
    )(mem_len, query_in, memory, w_query, w_key, w_value)


def solution(mesh):
    def local_step(query_in, memory, mem_len, w_query, w_key, w_value, w_out):
        n_batch, q_loc, d_model = query_in.shape
        n_heads, head_dim = w_query.shape[1], w_query.shape[2]
        core = lax.rem(lax.axis_index('seq'), 2)
        o1, s1, o2, s2 = attend(mem_len, query_in, memory, w_query, w_key, w_value)
        m1, l1, m2, l2 = s1[:, 0], s1[:, 1], s2[:, 0], s2[:, 1]
        m = jnp.maximum(m1, m2)
        f1, f2 = jnp.exp(m1 - m), jnp.exp(m2 - m)
        den = l1 * f1 + l2 * f2
        att = (o1 * f1[..., None] + o2 * f2[..., None]) / den[..., None]
        att = att.astype(BF16).reshape(n_heads // 2, n_batch, 2, q_loc, head_dim)
        mine = lax.dynamic_index_in_dim(att, core, 2, keepdims=False)
        other = lax.dynamic_index_in_dim(att, 1 - core, 2, keepdims=False)
        got = lax.ppermute(other, 'seq', [(0, 1), (1, 0), (2, 3), (3, 2)])
        heads = jnp.where(core == 0, jnp.concatenate([mine, got], 0), jnp.concatenate([got, mine], 0))
        return jnp.einsum('hbqd,hde->bqe', heads, w_out, preferred_element_type=F32).astype(BF16)

    return jax.shard_map(local_step, mesh=mesh, in_specs=(P('replica', 'seq', None), P('replica', 'seq', None), P('replica'), P(), P(), P(), P()), out_specs=P('replica', 'seq', None), check_vma=False)
```

```python
import functools
import math
import jax
import jax.numpy as jnp
from jax import lax
from jax.experimental import pallas as pl
from jax.experimental.pallas import tpu as pltpu
from jax.sharding import PartitionSpec as P

NEG_BIG = -1e30
BF16 = jnp.bfloat16
F32 = jnp.float32


def attend_kernel(len_ref, qin_hbm, mem_hbm, wq_hbm, wk_hbm, wv_hbm, wo_hbm,
                  out_hbm, oown_hbm, orecv_hbm, qown_hbm, qrecv_hbm,
                  x_buf, q_in, q_buf, raw_k, raw_v, w_a, w_b, kv_a, kv_b, o_buf, s_buf, s_recv,
                  c_rx, att_tx, out_buf, acc_buf,
                  x_sem, xr_send, xr_recv, qi_sem, qi_send, qi_recv, raw_sem,
                  q_send, q_recv, ql_sem, o_ssem, o_rsem, s_ssem, s_rsem, oo_sem,
                  wo_sem, c_sem, a_ssem, a_rsem, out_sem, free_sem):
    me = lax.axis_index('seq')
    chip = me // 2
    core = lax.rem(me, 2)
    partner = 2 * chip + (1 - core)
    cross = 2 * (1 - chip) + core
    n_batch, rows, d_model = mem_hbm.shape
    q_loc = qin_hbm.shape[1]
    head_dim = wq_hbm.shape[2]
    n_heads = wq_hbm.shape[1] // 2
    n_pairs = n_heads // 2
    head0 = core * n_heads
    half_q = 2 * q_loc
    n_q = n_batch * half_q
    per_att = d_model // head_dim
    scale = 1.0 / math.sqrt(head_dim)

    def to(dev):
        return dict(device_id={'seq': dev}, device_id_type=pl.DeviceIdType.MESH)

    def raw_copy(src, pair, k):
        return pltpu.make_async_copy(src.at[:, pl.ds(head0 + 2 * pair, 2), :], (raw_k, raw_v)[k], raw_sem.at[k])

    def x_local(b):
        return pltpu.make_async_copy(mem_hbm.at[b], x_buf.at[core, pl.ds(b * rows, rows)], x_sem.at[b])

    def x_remote(b):
        return pltpu.make_async_remote_copy(
            mem_hbm.at[b], x_buf.at[core, pl.ds(b * rows, rows)], xr_send.at[b], xr_recv.at[b], **to(partner))

    def q_copy(pair):
        sl = pl.ds(2 * pair, 2)
        return pltpu.make_async_remote_copy(qown_hbm.at[sl], qrecv_hbm.at[sl], q_send.at[pair], q_recv.at[pair], **to(cross))

    def q_store(pair):
        return pltpu.make_async_copy(q_buf.at[pair % 2], qown_hbm.at[pl.ds(2 * pair, 2)], ql_sem.at[pair % 2, 0])

    def q_loads(h, k):
        return (pltpu.make_async_copy(qown_hbm.at[h], q_buf.at[k, 0], ql_sem.at[k, 0]),
                pltpu.make_async_copy(qrecv_hbm.at[h], q_buf.at[k, 1], ql_sem.at[k, 1]))

    def o_copy(h, k):
        return pltpu.make_async_remote_copy(o_buf.at[k, 1], orecv_hbm.at[h], o_ssem.at[k], o_rsem.at[h], **to(cross))

    def o_piece(h, k, b):
        r = pl.ds(pl.multiple_of(b * half_q, half_q), half_q)
        return pltpu.make_async_remote_copy(o_buf.at[k, 1, r], orecv_hbm.at[h, r], o_ssem.at[k], o_rsem.at[h], **to(cross))

    def s_copy(h, k):
        return pltpu.make_async_remote_copy(s_buf.at[h, 1], s_recv.at[h], s_ssem.at[k], s_rsem.at[h], **to(cross))

    def oo_copy(h, k):
        return pltpu.make_async_copy(o_buf.at[k, 0], oown_hbm.at[h], oo_sem.at[k])

    qi_local = pltpu.make_async_copy(qin_hbm, q_in.at[:, core], qi_sem)
    raw_copy(wq_hbm, 0, 0).start()
    raw_copy(wq_hbm, 1, 1).start()
    qi_local.start()
    for b in range(n_batch):
        x_local(b).start()

    barrier = pltpu.get_barrier_semaphore()
    pl.semaphore_signal(barrier, inc=1, **to(partner))
    pl.semaphore_signal(barrier, inc=1, **to(cross))
    pl.semaphore_wait(barrier, 2)

    qi_remote = pltpu.make_async_remote_copy(qin_hbm, q_in.at[:, core], qi_send, qi_recv, **to(partner))
    qi_remote.start()
    for b in range(n_batch):
        x_remote(b).start()

    step = 128

    def relayout(raw, dst, sel, start, size):
        for i in range(size // step):
            r = pl.ds(pl.multiple_of(start + i * step, step), step)
            t = jnp.swapaxes(raw[r], 0, 1)
            dst[0, sel, r, :] = t[0]
            dst[1, sel, r, :] = t[1]

    half = d_model // 2

    raw_copy(wq_hbm, 0, 0).wait()

    def first_q(i, carry):
        relayout(raw_k, w_b, 0, i * half, half)
        return carry

    lax.fori_loop(0, 2, first_q, 0)
    raw_copy(wq_hbm, 2, 0).start()
    qi_local.wait()
    qi_remote.wait()
    for pair in range(n_pairs):
        k = (pair + 1) % 2
        last = pair + 1 == n_pairs
        src, idx = (wk_hbm, 0) if last else (wq_hbm, pair + 1)
        raw_copy(src, idx, k).wait()

        if pair >= 2:
            q_store(pair - 2).wait()
            q_copy(pair - 2).start()

        def q_step(j, carry, pair=pair, k=k, last=last):
            relayout((raw_k, raw_v)[k], w_a if last else w_b, 0 if last else k, j * half, half)
            q_rows = q_in[...].reshape(n_q, d_model)
            res = jnp.dot(q_rows, w_b[j, pair % 2], preferred_element_type=F32)
            q_buf[pair % 2, j] = res.astype(BF16)
            return carry

        lax.fori_loop(0, 2, q_step, 0)
        q_store(pair).start()
        if pair + 3 < n_pairs:
            raw_copy(wq_hbm, pair + 3, k).start()
        elif pair + 3 == n_pairs:
            raw_copy(wk_hbm, 0, k).start()
        elif pair + 2 == n_pairs:
            raw_copy(wv_hbm, 0, k).start()
    pl.semaphore_signal(free_sem, inc=1, **to(partner))
    raw_copy(wk_hbm, 1, 0).start()
    for pair in (n_pairs - 2, n_pairs - 1):
        q_store(pair).wait()
        q_copy(pair).start()
    raw_copy(wv_hbm, 0, 1).wait()

    def first_v(i, carry):
        relayout(raw_v, w_a, 1, i * half, half)
        return carry

    lax.fori_loop(0, 2, first_v, 0)
    raw_copy(wv_hbm, 1, 1).start()
    for b in range(n_batch):
        x_local(b).wait()

    def slices(b):
        return (pl.ds(pl.multiple_of(b * half_q, half_q), half_q), pl.ds(pl.multiple_of(b * rows, rows), rows))

    def weights(h, b, side, kv, k):
        q_sl, kv_sl = slices(b)
        k_b = kv[0, :, kv_sl, :].reshape(2 * rows, head_dim)
        s = lax.dot_general(q_buf[k, side, q_sl, :], k_b, (((1,), (1,)), ((), ())), preferred_element_type=F32) * scale
        pos = lax.broadcasted_iota(jnp.int32, s.shape, 1)
        s = jnp.where(pos < len_ref[b] - chip * (2 * rows), s, NEG_BIG)
        m = jnp.max(s, axis=1, keepdims=True)
        p = jnp.exp(s - m)
        l = jnp.sum(p, axis=1, keepdims=True)
        lane = lax.broadcasted_iota(jnp.int32, (half_q, 128), 1)
        s_buf[h, side, :, q_sl] = jnp.where(lane == 0, m, l).T[0:8]
        return p.astype(BF16)

    def weighted(p, b, side, kv, k):
        q_sl, kv_sl = slices(b)
        v_b = kv[1, :, kv_sl, :].reshape(2 * rows, head_dim)
        o_buf[k, side, q_sl, :] = jnp.dot(p, v_b, preferred_element_type=F32)

    n_tiles = 2 * n_batch
    part = d_model // n_batch
    big = n_batch * rows // 2

    def four_heads(sp, carry):
        for u in range(4):
            h = 4 * sp + u
            pair = 2 * sp + u // 2
            j = u % 2
            w_now, w_next = (w_a, w_b) if u < 2 else (w_b, w_a)
            kv_now, kv_prev = (kv_a, kv_b) if j == 0 else (kv_b, kv_a)
            k_prev = (u + 1) % 2
            h_prev = jnp.maximum(h - 1, 0)

            @pl.when(h >= 3)
            def _():
                o_copy(h - 3, k_prev).wait_send()
                s_copy(h - 3, k_prev).wait_send()
                oo_copy(h - 3, k_prev).wait()

            @pl.when(pair + 1 < n_pairs)
            def _(j=j, pair=pair):
                raw_copy((wk_hbm, wv_hbm)[j], pair + 1, j).wait()

            @pl.when(h >= 1)
            def _():
                for c in q_loads(h_prev, k_prev):
                    c.wait()

            def fetch_q(h=h, pair=pair, j=j):
                if j == 0:
                    q_copy(pair).wait()
                for c in q_loads(h, j):
                    c.start()

            if u == 0:
                pl.when(h >= 1)(fetch_q)
            else:
                fetch_q()

            def tile(t, c, fetch_q=fetch_q, u=u, h=h, j=j, w_now=w_now, w_next=w_next, kv_now=kv_now, kv_prev=kv_prev, k_prev=k_prev, h_prev=h_prev):
                if u == 0:
                    @pl.when((h == 0) & (t == n_batch // 2))
                    def _():
                        for b in range(n_batch):
                            x_remote(b).wait()
                        fetch_q()

                relayout((raw_k, raw_v)[j], w_next, j, t * part, part)
                p = [weights(h_prev, t, i, kv_prev, k_prev) for i in range(2)]
                side = lax.rem(core + t // 2, 2)
                r = pl.ds(pl.multiple_of(lax.rem(t, 2) * big, big), big)
                for sel in range(2):
                    kv_now[sel, side, r, :] = jnp.dot(x_buf[side, r, :], w_now[j, sel], preferred_element_type=F32).astype(BF16)
                    weighted(p[sel], t, sel, kv_prev, k_prev)

                @pl.when(h >= 1)
                def _():
                    o_piece(h - 1, k_prev, t).start()

                return c

            lax.fori_loop(0, n_batch, tile, 0)

            @pl.when(pair + 2 < n_pairs)
            def _(j=j, pair=pair):
                raw_copy((wk_hbm, wv_hbm)[j], pair + 2, j).start()

            @pl.when(h >= 1)
            def _():
                s_copy(h - 1, k_prev).start()
                oo_copy(h - 1, k_prev).start()
        return carry

    lax.fori_loop(0, n_heads // 4, four_heads, 0)

    n_wo = wo_hbm.shape[0] // 2
    wo_copies = [pltpu.make_async_copy(wo_hbm.at[pl.ds(i * n_wo, n_wo)], x_buf.at[i], wo_sem.at[i]) for i in range(2)]
    for c in wo_copies:
        c.start()

    final = n_heads - 1
    o_copy(final - 2, 1).wait_send()
    s_copy(final - 2, 1).wait_send()
    oo_copy(final - 2, 1).wait()

    for c in q_loads(final, 1):
        c.wait()

    def last_attention(b, c, side):
        weighted(weights(final, b, side, kv_b, 1), b, side, kv_b, 1)
        if side == 1:
            o_piece(final, 1, b).start()
        return c

    lax.fori_loop(0, n_batch, functools.partial(last_attention, side=1), 0)
    s_copy(final, 1).start()
    lax.fori_loop(0, n_batch, functools.partial(last_attention, side=0), 0)
    oo_copy(final, 1).start()

    half_rows = n_q // 2
    n_half = n_batch // 2

    def c_copies(h, i):
        r = pl.ds(i * half_rows, half_rows)
        return (pltpu.make_async_copy(oown_hbm.at[h, r], o_buf.at[0, 0, r], c_sem.at[0, i]),
                pltpu.make_async_copy(orecv_hbm.at[h, r], c_rx.at[i], c_sem.at[1, i]))

    def att_slot(h):
        hg = head0 + h
        return hg // per_att, pl.ds(pl.multiple_of(lax.rem(hg, per_att) * head_dim, head_dim), head_dim)

    def a_copy(h, k):
        side, lanes = att_slot(h)
        return pltpu.make_async_remote_copy(att_tx.at[k], q_in.at[:, side, :, lanes], a_ssem.at[k], a_rsem.at[h], **to(partner))

    def combine(h, k, following):
        t1, t2 = s_buf[h, 0].T, s_recv[h].T
        m1, l1, m2, l2 = t1[:, 0:1], t1[:, 1:2], t2[:, 0:1], t2[:, 1:2]
        m = jnp.maximum(m1, m2)
        f1, f2 = jnp.exp(m1 - m), jnp.exp(m2 - m)
        den = l1 * f1 + l2 * f2
        f1, f2 = f1 / den, f2 / den
        side, lanes = att_slot(h)
        for i in range(2):
            for c in c_copies(h, i):
                c.wait()
            for b in range(i * n_half, (i + 1) * n_half):
                r = slice(b * half_q, (b + 1) * half_q)
                rc = slice((b - i * n_half) * half_q, (b - i * n_half + 1) * half_q)
                res = (o_buf[0, 0, r, :] * f1[r] + c_rx[i, rc, :] * f2[r]).astype(BF16)
                lo, hi = res[:q_loc], res[q_loc:]
                q_in[b, side, :, lanes] = jnp.where(core == 0, lo, hi)
                att_tx[k, b] = jnp.where(core == 0, hi, lo)
            following(i)

    oo_copy(final - 1, 0).wait()
    o_copy(final - 1, 0).wait_send()
    s_copy(final - 1, 0).wait_send()
    pl.semaphore_wait(free_sem, 1)
    o_copy(0, 0).wait_recv()
    s_copy(0, 0).wait_recv()
    for i in range(2):
        for c in c_copies(0, i):
            c.start()

    def combine_step(h, carry):
        k = lax.rem(h, 2)

        @pl.when(h + 1 < final)
        def _():
            o_copy(h + 1, 0).wait_recv()
            s_copy(h + 1, 0).wait_recv()

        @pl.when(h >= 2)
        def _():
            a_copy(h - 2, k).wait_send()

        def following(i):
            @pl.when(h + 1 < final)
            def _():
                for c in c_copies(h + 1, i):
                    c.start()

        combine(h, k, following)
        a_copy(h, k).start()
        return carry

    lax.fori_loop(0, final, combine_step, 0)
    for c in wo_copies:
        c.wait()
    for h in range(final):
        a_copy(h, 0).wait_recv()

    width = out_buf.shape[2]
    n_out = n_batch * q_loc
    most = final * head_dim
    rest = 2 * n_wo - d_model
    n_cols = d_model // width

    def columns(n):
        return pl.ds(pl.multiple_of(n * width, width), width)

    def early_tile(n, carry):
        cols = columns(n)
        acc = jnp.dot(q_in[:, 0, :, 0:most].reshape(n_out, most), x_buf[0, 0:most, cols], preferred_element_type=F32)
        acc += jnp.dot(q_in[:, 0, :, n_wo:].reshape(n_out, d_model - n_wo), x_buf[1, 0:d_model - n_wo, cols], preferred_element_type=F32)
        acc += jnp.dot(q_in[:, 1, :, 0:rest - head_dim].reshape(n_out, rest - head_dim), x_buf[1, d_model - n_wo:most, cols], preferred_element_type=F32)
        acc_buf[:, cols] = acc
        return carry

    lax.fori_loop(0, n_cols, early_tile, 0)
    k = final % 2
    oo_copy(final, 1).wait()
    o_copy(final, 1).wait_send()
    s_copy(final, 1).wait_send()
    a_copy(final - 2, k).wait_send()
    o_copy(final, 1).wait_recv()
    s_copy(final, 1).wait_recv()
    for i in range(2):
        for c in c_copies(final, i):
            c.start()
    combine(final, k, lambda i: None)
    a_copy(final, k).start()
    a_copy(final - 1, 1 - k).wait_send()
    a_copy(final, k).wait_send()
    a_copy(final, k).wait_recv()

    def out_copy(n, k):
        return pltpu.make_async_copy(out_buf.at[k], out_hbm.at[:, columns(n)], out_sem.at[k])

    def out_tile(n, carry):
        k = lax.rem(n, 2)

        @pl.when(n >= 2)
        def _():
            out_copy(n - 2, k).wait()

        cols = columns(n)
        acc = acc_buf[:, cols] + jnp.dot(q_in[:, 0, :, most:n_wo].reshape(n_out, head_dim), x_buf[0, most:n_wo, cols], preferred_element_type=F32)
        acc += jnp.dot(q_in[:, 1, :, rest - head_dim:rest].reshape(n_out, head_dim), x_buf[1, most:n_wo, cols], preferred_element_type=F32)
        out_buf[k] = acc.astype(BF16)
        out_copy(n, k).start()
        return carry

    lax.fori_loop(0, n_cols, out_tile, 0)
    for n in (n_cols - 2, n_cols - 1):
        out_copy(n, n % 2).wait()


def solution(mesh):
    def local_step(query_in, memory, mem_len, w_query, w_key, w_value, w_out):
        n_batch, q_loc, d_model = query_in.shape
        mem_local = memory.shape[1]
        head_dim = w_query.shape[2]
        n_heads = w_query.shape[1] // 2
        n_pairs = n_heads // 2
        n_q = n_batch * 2 * q_loc
        out_width = 512
        any_spec = pl.BlockSpec(memory_space=pl.ANY)
        part = jax.ShapeDtypeStruct((n_heads, n_q, head_dim), F32)
        dma = pltpu.SemaphoreType.DMA
        q_part = jax.ShapeDtypeStruct((n_heads, n_q, head_dim), BF16)
        out = pl.pallas_call(
            attend_kernel,
            out_shape=(jax.ShapeDtypeStruct((n_batch * q_loc, d_model), BF16), part, part, q_part, q_part),
            in_specs=[pl.BlockSpec(memory_space=pltpu.SMEM)] + [any_spec] * 6,
            out_specs=(any_spec,) * 5,
            scratch_shapes=[
                pltpu.VMEM((2, n_batch * mem_local, d_model), BF16),
                pltpu.VMEM((n_batch, 2, q_loc, d_model), BF16),
                pltpu.VMEM((2, 2, n_q, head_dim), BF16),
                pltpu.VMEM((d_model, 2, head_dim), BF16),
                pltpu.VMEM((d_model, 2, head_dim), BF16),
                pltpu.VMEM((2, 2, d_model, head_dim), BF16),
                pltpu.VMEM((2, 2, d_model, head_dim), BF16),
                pltpu.VMEM((2, 2, n_batch * mem_local, head_dim), BF16),
                pltpu.VMEM((2, 2, n_batch * mem_local, head_dim), BF16),
                pltpu.VMEM((2, 2, n_q, head_dim), F32),
                pltpu.VMEM((n_heads, 2, 8, n_q), F32),
                pltpu.VMEM((n_heads, 8, n_q), F32),
                pltpu.VMEM((2, n_q // 2, head_dim), F32),
                pltpu.VMEM((2, n_batch, q_loc, head_dim), BF16),
                pltpu.VMEM((2, n_batch * q_loc, out_width), BF16),
                pltpu.VMEM((n_batch * q_loc, d_model), F32),
                dma((n_batch,)), dma((n_batch,)), dma((n_batch,)), dma, dma, dma, dma((2,)),
                dma((n_pairs,)), dma((n_pairs,)), dma((2, 2)), dma((2,)), dma((n_heads,)), dma((2,)), dma((n_heads,)), dma((2,)),
                dma((2,)), dma((2, 2)), dma((2,)), dma((n_heads,)), dma((2,)), pltpu.SemaphoreType.REGULAR,
            ],
            compiler_params=pltpu.CompilerParams(collective_id=0, has_side_effects=True, vmem_limit_bytes=67043328),
        )(mem_len, query_in, memory, w_query, w_key, w_value, w_out.reshape(2 * n_heads * head_dim, d_model))[0]
        return out.reshape(n_batch, q_loc, d_model)

    return jax.shard_map(local_step, mesh=mesh, in_specs=(P('replica', 'seq', None), P('replica', 'seq', None), P('replica'), P(), P(), P(), P()), out_specs=P('replica', 'seq', None), check_vma=False)
```

```python
import functools
import math
import jax
import jax.numpy as jnp
from jax import lax
from jax.experimental import pallas as pl
from jax.experimental.pallas import tpu as pltpu
from jax.sharding import PartitionSpec as P

NEG_BIG = -1e30
BF16 = jnp.bfloat16
F32 = jnp.float32


def attend_kernel(len_ref, qin_hbm, mem_hbm, wq_hbm, wk_hbm, wv_hbm, wo_hbm,
                  out_hbm, oown_hbm, orecv_hbm, qown_hbm, qrecv_hbm,
                  x_buf, q_in, q_buf, raw_k, raw_v, w_a, w_b, kv_a, kv_b, o_buf, s_buf, s_recv,
                  c_rx, att_tx, out_buf, acc_buf,
                  x_sem, xr_send, xr_recv, qi_sem, qi_send, qi_recv, raw_sem,
                  q_send, q_recv, ql_sem, o_ssem, o_rsem, s_ssem, s_rsem, oo_sem,
                  wo_sem, c_sem, a_ssem, a_rsem, out_sem, free_sem):
    me = lax.axis_index('seq')
    chip = me // 2
    core = lax.rem(me, 2)
    partner = 2 * chip + (1 - core)
    cross = 2 * (1 - chip) + core
    n_batch, rows, d_model = mem_hbm.shape
    q_loc = qin_hbm.shape[1]
    head_dim = wq_hbm.shape[2]
    n_heads = wq_hbm.shape[1] // 2
    n_pairs = n_heads // 2
    head0 = core * n_heads
    half_q = 2 * q_loc
    n_q = n_batch * half_q
    per_att = d_model // head_dim
    scale = 1.0 / math.sqrt(head_dim)

    def to(dev):
        return dict(device_id={'seq': dev}, device_id_type=pl.DeviceIdType.MESH)

    def raw_copy(src, pair, k):
        return pltpu.make_async_copy(src.at[:, pl.ds(head0 + 2 * pair, 2), :], (raw_k, raw_v)[k], raw_sem.at[k])

    def x_local(b):
        return pltpu.make_async_copy(mem_hbm.at[b], x_buf.at[core, pl.ds(b * rows, rows)], x_sem.at[b])

    def x_remote(b):
        return pltpu.make_async_remote_copy(
            mem_hbm.at[b], x_buf.at[core, pl.ds(b * rows, rows)], xr_send.at[b], xr_recv.at[b], **to(partner))

    def q_copy(pair):
        sl = pl.ds(2 * pair, 2)
        return pltpu.make_async_remote_copy(qown_hbm.at[sl], qrecv_hbm.at[sl], q_send.at[pair], q_recv.at[pair], **to(cross))

    def q_store(pair):
        return pltpu.make_async_copy(q_buf.at[pair % 2], qown_hbm.at[pl.ds(2 * pair, 2)], ql_sem.at[pair % 2, 0])

    def q_loads(h, k):
        return (pltpu.make_async_copy(qown_hbm.at[h], q_buf.at[k, 0], ql_sem.at[k, 0]),
                pltpu.make_async_copy(qrecv_hbm.at[h], q_buf.at[k, 1], ql_sem.at[k, 1]))

    def o_copy(h, k):
        return pltpu.make_async_remote_copy(o_buf.at[k, 1], orecv_hbm.at[h], o_ssem.at[k], o_rsem.at[h], **to(cross))

    def o_piece(h, k, b):
        r = pl.ds(pl.multiple_of(b * half_q, half_q), half_q)
        return pltpu.make_async_remote_copy(o_buf.at[k, 1, r], orecv_hbm.at[h, r], o_ssem.at[k], o_rsem.at[h], **to(cross))

    def s_copy(h, k):
        return pltpu.make_async_remote_copy(s_buf.at[h, 1], s_recv.at[h], s_ssem.at[k], s_rsem.at[h], **to(cross))

    def oo_copy(h, k):
        return pltpu.make_async_copy(o_buf.at[k, 0], oown_hbm.at[h], oo_sem.at[k])

    qi_local = pltpu.make_async_copy(qin_hbm, q_in.at[:, core], qi_sem)
    raw_copy(wq_hbm, 0, 0).start()
    raw_copy(wq_hbm, 1, 1).start()
    qi_local.start()
    for b in range(n_batch):
        x_local(b).start()

    barrier = pltpu.get_barrier_semaphore()
    pl.semaphore_signal(barrier, inc=1, **to(partner))
    pl.semaphore_signal(barrier, inc=1, **to(cross))
    pl.semaphore_wait(barrier, 2)

    qi_remote = pltpu.make_async_remote_copy(qin_hbm, q_in.at[:, core], qi_send, qi_recv, **to(partner))
    qi_remote.start()
    for b in range(n_batch):
        x_remote(b).start()

    step = 128

    def relayout(raw, dst, sel, start, size):
        for i in range(size // step):
            r = pl.ds(pl.multiple_of(start + i * step, step), step)
            t = jnp.swapaxes(raw[r], 0, 1)
            dst[0, sel, r, :] = t[0]
            dst[1, sel, r, :] = t[1]

    half = d_model // 2

    raw_copy(wq_hbm, 0, 0).wait()

    def first_q(i, carry):
        relayout(raw_k, w_b, 0, i * half, half)
        return carry

    lax.fori_loop(0, 2, first_q, 0)
    raw_copy(wq_hbm, 2, 0).start()
    qi_local.wait()
    qi_remote.wait()
    for pair in range(n_pairs):
        k = (pair + 1) % 2
        last = pair + 1 == n_pairs
        src, idx = (wk_hbm, 0) if last else (wq_hbm, pair + 1)
        raw_copy(src, idx, k).wait()

        if pair >= 2:
            q_store(pair - 2).wait()
            q_copy(pair - 2).start()

        def q_next(j, carry, k=k, last=last):
            relayout((raw_k, raw_v)[k], w_a if last else w_b, 0 if last else k, j * half, half)
            return carry

        def q_step(j, carry, pair=pair):
            q_rows = q_in[...].reshape(n_q, d_model)
            res = jnp.dot(q_rows, w_b[j, pair % 2], preferred_element_type=F32)
            q_buf[pair % 2, j] = res.astype(BF16)
            return carry

        lax.fori_loop(0, 2, q_next, 0)
        lax.fori_loop(0, 2, q_step, 0)
        q_store(pair).start()
        if pair + 3 < n_pairs:
            raw_copy(wq_hbm, pair + 3, k).start()
        elif pair + 3 == n_pairs:
            raw_copy(wk_hbm, 0, k).start()
        elif pair + 2 == n_pairs:
            raw_copy(wv_hbm, 0, k).start()
    pl.semaphore_signal(free_sem, inc=1, **to(partner))
    raw_copy(wk_hbm, 1, 0).start()
    for pair in (n_pairs - 2, n_pairs - 1):
        q_store(pair).wait()
        q_copy(pair).start()
    raw_copy(wv_hbm, 0, 1).wait()

    def first_v(i, carry):
        relayout(raw_v, w_a, 1, i * half, half)
        return carry

    lax.fori_loop(0, 2, first_v, 0)
    raw_copy(wv_hbm, 1, 1).start()
    for b in range(n_batch):
        x_local(b).wait()

    def slices(b):
        return (pl.ds(pl.multiple_of(b * half_q, half_q), half_q), pl.ds(pl.multiple_of(b * rows, rows), rows))

    def weights(h, b, side, kv, k):
        q_sl, kv_sl = slices(b)
        k_b = kv[0, :, kv_sl, :].reshape(2 * rows, head_dim)
        s = lax.dot_general(q_buf[k, side, q_sl, :], k_b, (((1,), (1,)), ((), ())), preferred_element_type=F32) * scale
        pos = lax.broadcasted_iota(jnp.int32, s.shape, 1)
        s = jnp.where(pos < len_ref[b] - chip * (2 * rows), s, NEG_BIG)
        m = jnp.max(s, axis=1, keepdims=True)
        p = jnp.exp(s - m)
        l = jnp.sum(p, axis=1, keepdims=True)
        lane = lax.broadcasted_iota(jnp.int32, (half_q, 128), 1)
        s_buf[h, side, :, q_sl] = jnp.where(lane == 0, m, l).T[0:8]
        return p.astype(BF16)

    def weighted(p, b, side, kv, k):
        q_sl, kv_sl = slices(b)
        v_b = kv[1, :, kv_sl, :].reshape(2 * rows, head_dim)
        o_buf[k, side, q_sl, :] = jnp.dot(p, v_b, preferred_element_type=F32)

    n_tiles = 2 * n_batch
    part = d_model // n_batch
    big = n_batch * rows // 2

    def four_heads(sp, carry):
        for u in range(4):
            h = 4 * sp + u
            pair = 2 * sp + u // 2
            j = u % 2
            w_now, w_next = (w_a, w_b) if u < 2 else (w_b, w_a)
            kv_now, kv_prev = (kv_a, kv_b) if j == 0 else (kv_b, kv_a)
            k_prev = (u + 1) % 2
            h_prev = jnp.maximum(h - 1, 0)

            @pl.when(h >= 3)
            def _():
                o_copy(h - 3, k_prev).wait_send()
                s_copy(h - 3, k_prev).wait_send()
                oo_copy(h - 3, k_prev).wait()

            @pl.when(pair + 1 < n_pairs)
            def _(j=j, pair=pair):
                raw_copy((wk_hbm, wv_hbm)[j], pair + 1, j).wait()

            @pl.when(h >= 1)
            def _():
                for c in q_loads(h_prev, k_prev):
                    c.wait()

            def fetch_q(h=h, pair=pair, j=j):
                if j == 0:
                    q_copy(pair).wait()
                for c in q_loads(h, j):
                    c.start()

            if u == 0:
                pl.when(h >= 1)(fetch_q)
            else:
                fetch_q()

            def tile(t, c, fetch_q=fetch_q, pair=pair, u=u, h=h, j=j, w_now=w_now, w_next=w_next, kv_now=kv_now, kv_prev=kv_prev, k_prev=k_prev, h_prev=h_prev):
                if u == 0:
                    @pl.when((h == 0) & (t == n_batch // 2))
                    def _():
                        for b in range(n_batch):
                            x_remote(b).wait()
                        fetch_q()

                @pl.when(pair + 1 < n_pairs)
                def _():
                    relayout((raw_k, raw_v)[j], w_next, j, t * part, part)

                p = [weights(h_prev, t, i, kv_prev, k_prev) for i in range(2)]
                side = lax.rem(core + t // 2, 2)
                r = pl.ds(pl.multiple_of(lax.rem(t, 2) * big, big), big)
                for sel in range(2):
                    kv_now[sel, side, r, :] = jnp.dot(x_buf[side, r, :], w_now[j, sel], preferred_element_type=F32).astype(BF16)
                    weighted(p[sel], t, sel, kv_prev, k_prev)

                @pl.when(h >= 1)
                def _():
                    o_piece(h - 1, k_prev, t).start()

                return c

            lax.fori_loop(0, n_batch, tile, 0)

            @pl.when(pair + 2 < n_pairs)
            def _(j=j, pair=pair):
                raw_copy((wk_hbm, wv_hbm)[j], pair + 2, j).start()

            @pl.when(h >= 1)
            def _():
                s_copy(h - 1, k_prev).start()
                oo_copy(h - 1, k_prev).start()
        return carry

    lax.fori_loop(0, n_heads // 4, four_heads, 0)

    n_wo = wo_hbm.shape[0] // 2
    wo_copies = [pltpu.make_async_copy(wo_hbm.at[pl.ds(i * n_wo, n_wo)], x_buf.at[i], wo_sem.at[i]) for i in range(2)]
    for c in wo_copies:
        c.start()

    final = n_heads - 1
    o_copy(final - 2, 1).wait_send()
    s_copy(final - 2, 1).wait_send()
    oo_copy(final - 2, 1).wait()

    for c in q_loads(final, 1):
        c.wait()

    def last_attention(b, c, side):
        weighted(weights(final, b, side, kv_b, 1), b, side, kv_b, 1)
        if side == 1:
            o_piece(final, 1, b).start()
        return c

    lax.fori_loop(0, n_batch, functools.partial(last_attention, side=1), 0)
    s_copy(final, 1).start()
    lax.fori_loop(0, n_batch, functools.partial(last_attention, side=0), 0)
    oo_copy(final, 1).start()

    half_rows = n_q // 2
    n_half = n_batch // 2

    def c_copies(h, i):
        r = pl.ds(i * half_rows, half_rows)
        return (pltpu.make_async_copy(oown_hbm.at[h, r], o_buf.at[0, 0, r], c_sem.at[0, i]),
                pltpu.make_async_copy(orecv_hbm.at[h, r], c_rx.at[i], c_sem.at[1, i]))

    def att_slot(h):
        hg = head0 + h
        return hg // per_att, pl.ds(pl.multiple_of(lax.rem(hg, per_att) * head_dim, head_dim), head_dim)

    def a_copy(h, k):
        side, lanes = att_slot(h)
        return pltpu.make_async_remote_copy(att_tx.at[k], q_in.at[:, side, :, lanes], a_ssem.at[k], a_rsem.at[h], **to(partner))

    def combine(h, k, following):
        t1, t2 = s_buf[h, 0].T, s_recv[h].T
        m1, l1, m2, l2 = t1[:, 0:1], t1[:, 1:2], t2[:, 0:1], t2[:, 1:2]
        m = jnp.maximum(m1, m2)
        f1, f2 = jnp.exp(m1 - m), jnp.exp(m2 - m)
        den = l1 * f1 + l2 * f2
        f1, f2 = f1 / den, f2 / den
        side, lanes = att_slot(h)
        for i in range(2):
            for c in c_copies(h, i):
                c.wait()
            for b in range(i * n_half, (i + 1) * n_half):
                r = slice(b * half_q, (b + 1) * half_q)
                rc = slice((b - i * n_half) * half_q, (b - i * n_half + 1) * half_q)
                res = (o_buf[0, 0, r, :] * f1[r] + c_rx[i, rc, :] * f2[r]).astype(BF16)
                lo, hi = res[:q_loc], res[q_loc:]
                q_in[b, side, :, lanes] = jnp.where(core == 0, lo, hi)
                att_tx[k, b] = jnp.where(core == 0, hi, lo)
            following(i)

    oo_copy(final - 1, 0).wait()
    o_copy(final - 1, 0).wait_send()
    s_copy(final - 1, 0).wait_send()
    pl.semaphore_wait(free_sem, 1)
    o_copy(0, 0).wait_recv()
    s_copy(0, 0).wait_recv()
    for i in range(2):
        for c in c_copies(0, i):
            c.start()

    def combine_step(h, carry):
        k = lax.rem(h, 2)

        @pl.when(h + 1 < final)
        def _():
            o_copy(h + 1, 0).wait_recv()
            s_copy(h + 1, 0).wait_recv()

        @pl.when(h >= 2)
        def _():
            a_copy(h - 2, k).wait_send()

        def following(i):
            @pl.when(h + 1 < final)
            def _():
                for c in c_copies(h + 1, i):
                    c.start()

        combine(h, k, following)
        a_copy(h, k).start()
        return carry

    lax.fori_loop(0, final, combine_step, 0)
    for c in wo_copies:
        c.wait()
    for h in range(final):
        a_copy(h, 0).wait_recv()

    width = out_buf.shape[2]
    n_out = n_batch * q_loc
    most = final * head_dim
    rest = 2 * n_wo - d_model
    n_cols = d_model // width

    def columns(n):
        return pl.ds(pl.multiple_of(n * width, width), width)

    def early_tile(n, carry):
        cols = columns(n)
        acc = jnp.dot(q_in[:, 0, :, 0:most].reshape(n_out, most), x_buf[0, 0:most, cols], preferred_element_type=F32)
        acc += jnp.dot(q_in[:, 0, :, n_wo:].reshape(n_out, d_model - n_wo), x_buf[1, 0:d_model - n_wo, cols], preferred_element_type=F32)
        acc += jnp.dot(q_in[:, 1, :, 0:rest - head_dim].reshape(n_out, rest - head_dim), x_buf[1, d_model - n_wo:most, cols], preferred_element_type=F32)
        acc_buf[:, cols] = acc
        return carry

    lax.fori_loop(0, n_cols, early_tile, 0)
    k = final % 2
    oo_copy(final, 1).wait()
    o_copy(final, 1).wait_send()
    s_copy(final, 1).wait_send()
    a_copy(final - 2, k).wait_send()
    o_copy(final, 1).wait_recv()
    s_copy(final, 1).wait_recv()
    for i in range(2):
        for c in c_copies(final, i):
            c.start()
    combine(final, k, lambda i: None)
    a_copy(final, k).start()
    a_copy(final - 1, 1 - k).wait_send()
    a_copy(final, k).wait_send()
    a_copy(final, k).wait_recv()

    def out_copy(n, k):
        return pltpu.make_async_copy(out_buf.at[k], out_hbm.at[:, columns(n)], out_sem.at[k])

    def out_tile(n, carry):
        k = lax.rem(n, 2)

        @pl.when(n >= 2)
        def _():
            out_copy(n - 2, k).wait()

        cols = columns(n)
        acc = acc_buf[:, cols] + jnp.dot(q_in[:, 0, :, most:n_wo].reshape(n_out, head_dim), x_buf[0, most:n_wo, cols], preferred_element_type=F32)
        acc += jnp.dot(q_in[:, 1, :, rest - head_dim:rest].reshape(n_out, head_dim), x_buf[1, most:n_wo, cols], preferred_element_type=F32)
        out_buf[k] = acc.astype(BF16)
        out_copy(n, k).start()
        return carry

    lax.fori_loop(0, n_cols, out_tile, 0)
    for n in (n_cols - 2, n_cols - 1):
        out_copy(n, n % 2).wait()


def solution(mesh):
    def local_step(query_in, memory, mem_len, w_query, w_key, w_value, w_out):
        n_batch, q_loc, d_model = query_in.shape
        mem_local = memory.shape[1]
        head_dim = w_query.shape[2]
        n_heads = w_query.shape[1] // 2
        n_pairs = n_heads // 2
        n_q = n_batch * 2 * q_loc
        out_width = 512
        any_spec = pl.BlockSpec(memory_space=pl.ANY)
        part = jax.ShapeDtypeStruct((n_heads, n_q, head_dim), F32)
        dma = pltpu.SemaphoreType.DMA
        q_part = jax.ShapeDtypeStruct((n_heads, n_q, head_dim), BF16)
        out = pl.pallas_call(
            attend_kernel,
            out_shape=(jax.ShapeDtypeStruct((n_batch * q_loc, d_model), BF16), part, part, q_part, q_part),
            in_specs=[pl.BlockSpec(memory_space=pltpu.SMEM)] + [any_spec] * 6,
            out_specs=(any_spec,) * 5,
            scratch_shapes=[
                pltpu.VMEM((2, n_batch * mem_local, d_model), BF16),
                pltpu.VMEM((n_batch, 2, q_loc, d_model), BF16),
                pltpu.VMEM((2, 2, n_q, head_dim), BF16),
                pltpu.VMEM((d_model, 2, head_dim), BF16),
                pltpu.VMEM((d_model, 2, head_dim), BF16),
                pltpu.VMEM((2, 2, d_model, head_dim), BF16),
                pltpu.VMEM((2, 2, d_model, head_dim), BF16),
                pltpu.VMEM((2, 2, n_batch * mem_local, head_dim), BF16),
                pltpu.VMEM((2, 2, n_batch * mem_local, head_dim), BF16),
                pltpu.VMEM((2, 2, n_q, head_dim), F32),
                pltpu.VMEM((n_heads, 2, 8, n_q), F32),
                pltpu.VMEM((n_heads, 8, n_q), F32),
                pltpu.VMEM((2, n_q // 2, head_dim), F32),
                pltpu.VMEM((2, n_batch, q_loc, head_dim), BF16),
                pltpu.VMEM((2, n_batch * q_loc, out_width), BF16),
                pltpu.VMEM((n_batch * q_loc, d_model), F32),
                dma((n_batch,)), dma((n_batch,)), dma((n_batch,)), dma, dma, dma, dma((2,)),
                dma((n_pairs,)), dma((n_pairs,)), dma((2, 2)), dma((2,)), dma((n_heads,)), dma((2,)), dma((n_heads,)), dma((2,)),
                dma((2,)), dma((2, 2)), dma((2,)), dma((n_heads,)), dma((2,)), pltpu.SemaphoreType.REGULAR,
            ],
            compiler_params=pltpu.CompilerParams(collective_id=0, has_side_effects=True, vmem_limit_bytes=67043328),
        )(mem_len, query_in, memory, w_query, w_key, w_value, w_out.reshape(2 * n_heads * head_dim, d_model))[0]
        return out.reshape(n_batch, q_loc, d_model)

    return jax.shard_map(local_step, mesh=mesh, in_specs=(P('replica', 'seq', None), P('replica', 'seq', None), P('replica'), P(), P(), P(), P()), out_specs=P('replica', 'seq', None), check_vma=False)
```

```python
import functools
import math
import jax
import jax.numpy as jnp
from jax import lax
from jax.experimental import pallas as pl
from jax.experimental.pallas import tpu as pltpu
from jax.sharding import PartitionSpec as P

NEG_BIG = -1e30
BF16 = jnp.bfloat16
F32 = jnp.float32


def attend_kernel(len_ref, qin_hbm, mem_hbm, wq_hbm, wk_hbm, wv_hbm, wo_hbm,
                  out_hbm, oown_hbm, orecv_hbm, qown_hbm, qrecv_hbm,
                  x_buf, q_in, q_buf, raw_k, raw_v, w_a, w_b, kv_a, kv_b, o_buf, s_buf, s_recv,
                  c_rx, att_tx, out_buf, acc_buf,
                  x_sem, xr_send, xr_recv, qi_sem, qi_send, qi_recv, raw_sem,
                  q_send, q_recv, ql_sem, o_ssem, o_rsem, s_ssem, s_rsem, oo_sem,
                  wo_sem, c_sem, a_ssem, a_rsem, out_sem, free_sem):
    me = lax.axis_index('seq')
    chip = me // 2
    core = lax.rem(me, 2)
    partner = 2 * chip + (1 - core)
    cross = 2 * (1 - chip) + core
    n_batch, rows, d_model = mem_hbm.shape
    q_loc = qin_hbm.shape[1]
    head_dim = wq_hbm.shape[2]
    n_heads = wq_hbm.shape[1] // 2
    n_pairs = n_heads // 2
    head0 = core * n_heads
    half_q = 2 * q_loc
    n_q = n_batch * half_q
    per_att = d_model // head_dim
    scale = 1.0 / math.sqrt(head_dim)

    def to(dev):
        return dict(device_id={'seq': dev}, device_id_type=pl.DeviceIdType.MESH)

    def raw_copy(src, pair, k):
        return pltpu.make_async_copy(src.at[:, pl.ds(head0 + 2 * pair, 2), :], (raw_k, raw_v)[k], raw_sem.at[k])

    def x_local(b):
        return pltpu.make_async_copy(mem_hbm.at[b], x_buf.at[core, pl.ds(b * rows, rows)], x_sem.at[b])

    def x_remote(b):
        return pltpu.make_async_remote_copy(
            mem_hbm.at[b], x_buf.at[core, pl.ds(b * rows, rows)], xr_send.at[b], xr_recv.at[b], **to(partner))

    def q_copy(pair):
        sl = pl.ds(2 * pair, 2)
        return pltpu.make_async_remote_copy(qown_hbm.at[sl], qrecv_hbm.at[sl], q_send.at[pair], q_recv.at[pair], **to(cross))

    def q_store(pair):
        return pltpu.make_async_copy(q_buf.at[pair % 2], qown_hbm.at[pl.ds(2 * pair, 2)], ql_sem.at[pair % 2, 0])

    def q_loads(h, k):
        return (pltpu.make_async_copy(qown_hbm.at[h], q_buf.at[k, 0], ql_sem.at[k, 0]),
                pltpu.make_async_copy(qrecv_hbm.at[h], q_buf.at[k, 1], ql_sem.at[k, 1]))

    def o_copy(h, k):
        return pltpu.make_async_remote_copy(o_buf.at[k, 1], orecv_hbm.at[h], o_ssem.at[k], o_rsem.at[h], **to(cross))

    def o_piece(h, k, b):
        r = pl.ds(pl.multiple_of(b * half_q, half_q), half_q)
        return pltpu.make_async_remote_copy(o_buf.at[k, 1, r], orecv_hbm.at[h, r], o_ssem.at[k], o_rsem.at[h], **to(cross))

    def s_copy(h, k):
        return pltpu.make_async_remote_copy(s_buf.at[h, 1], s_recv.at[h], s_ssem.at[k], s_rsem.at[h], **to(cross))

    def oo_copy(h, k):
        return pltpu.make_async_copy(o_buf.at[k, 0], oown_hbm.at[h], oo_sem.at[k])

    qi_local = pltpu.make_async_copy(qin_hbm, q_in.at[:, core], qi_sem)
    raw_copy(wq_hbm, 0, 0).start()
    raw_copy(wq_hbm, 1, 1).start()
    qi_local.start()
    for b in range(n_batch):
        x_local(b).start()

    barrier = pltpu.get_barrier_semaphore()
    pl.semaphore_signal(barrier, inc=1, **to(partner))
    pl.semaphore_signal(barrier, inc=1, **to(cross))
    pl.semaphore_wait(barrier, 2)

    qi_remote = pltpu.make_async_remote_copy(qin_hbm, q_in.at[:, core], qi_send, qi_recv, **to(partner))
    qi_remote.start()
    for b in range(n_batch):
        x_remote(b).start()

    step = 128

    def relayout(raw, dst, sel, start, size):
        for i in range(size // step):
            r = pl.ds(pl.multiple_of(start + i * step, step), step)
            t = jnp.swapaxes(raw[r], 0, 1)
            dst[0, sel, r, :] = t[0]
            dst[1, sel, r, :] = t[1]

    half = d_model // 2

    raw_copy(wq_hbm, 0, 0).wait()

    def first_q(i, carry):
        relayout(raw_k, w_b, 0, i * half, half)
        return carry

    lax.fori_loop(0, 2, first_q, 0)
    raw_copy(wq_hbm, 2, 0).start()
    qi_local.wait()
    qi_remote.wait()
    for pair in range(n_pairs):
        k = (pair + 1) % 2
        last = pair + 1 == n_pairs
        src, idx = (wk_hbm, 0) if last else (wq_hbm, pair + 1)
        raw_copy(src, idx, k).wait()

        if pair >= 2:
            q_store(pair - 2).wait()
            q_copy(pair - 2).start()

        def q_next(j, carry, k=k, last=last):
            relayout((raw_k, raw_v)[k], w_a if last else w_b, 0 if last else k, j * half, half)
            return carry

        def q_step(j, carry, pair=pair):
            q_rows = q_in[...].reshape(n_q, d_model)
            res = jnp.dot(q_rows, w_b[j, pair % 2], preferred_element_type=F32)
            q_buf[pair % 2, j] = res.astype(BF16)
            return carry

        lax.fori_loop(0, 2, q_next, 0)
        lax.fori_loop(0, 2, q_step, 0)
        q_store(pair).start()
        if pair + 3 < n_pairs:
            raw_copy(wq_hbm, pair + 3, k).start()
        elif pair + 3 == n_pairs:
            raw_copy(wk_hbm, 0, k).start()
        elif pair + 2 == n_pairs:
            raw_copy(wv_hbm, 0, k).start()
    pl.semaphore_signal(free_sem, inc=1, **to(partner))
    raw_copy(wk_hbm, 1, 0).start()
    for pair in (n_pairs - 2, n_pairs - 1):
        q_store(pair).wait()
        q_copy(pair).start()
    raw_copy(wv_hbm, 0, 1).wait()

    def first_v(i, carry):
        relayout(raw_v, w_a, 1, i * half, half)
        return carry

    lax.fori_loop(0, 2, first_v, 0)
    raw_copy(wv_hbm, 1, 1).start()
    for b in range(n_batch):
        x_local(b).wait()

    def slices(b):
        return (pl.ds(pl.multiple_of(b * half_q, half_q), half_q), pl.ds(pl.multiple_of(b * rows, rows), rows))

    def weights(h, b, side, kv, k):
        q_sl, kv_sl = slices(b)
        k_b = kv[0, :, kv_sl, :].reshape(2 * rows, head_dim)
        s = lax.dot_general(q_buf[k, side, q_sl, :], k_b, (((1,), (1,)), ((), ())), preferred_element_type=F32) * scale
        pos = lax.broadcasted_iota(jnp.int32, s.shape, 1)
        s = jnp.where(pos < len_ref[b] - chip * (2 * rows), s, NEG_BIG)
        m = jnp.max(s, axis=1, keepdims=True)
        p = jnp.exp(s - m)
        l = jnp.sum(p, axis=1, keepdims=True)
        lane = lax.broadcasted_iota(jnp.int32, (half_q, 128), 1)
        s_buf[h, side, :, q_sl] = jnp.where(lane == 0, m, l).T[0:8]
        return p.astype(BF16)

    def weighted(p, b, side, kv, k):
        q_sl, kv_sl = slices(b)
        v_b = kv[1, :, kv_sl, :].reshape(2 * rows, head_dim)
        o_buf[k, side, q_sl, :] = jnp.dot(p, v_b, preferred_element_type=F32)

    n_tiles = 2 * n_batch
    part = d_model // n_batch
    big = n_batch * rows // 2

    def four_heads(sp, carry):
        for u in range(4):
            h = 4 * sp + u
            pair = 2 * sp + u // 2
            j = u % 2
            w_now, w_next = (w_a, w_b) if u < 2 else (w_b, w_a)
            kv_now, kv_prev = (kv_a, kv_b) if j == 0 else (kv_b, kv_a)
            k_prev = (u + 1) % 2
            h_prev = jnp.maximum(h - 1, 0)

            @pl.when(h >= 3)
            def _():
                o_copy(h - 3, k_prev).wait_send()
                s_copy(h - 3, k_prev).wait_send()
                oo_copy(h - 3, k_prev).wait()

            @pl.when(pair + 1 < n_pairs)
            def _(j=j, pair=pair):
                raw_copy((wk_hbm, wv_hbm)[j], pair + 1, j).wait()

            @pl.when(h >= 1)
            def _():
                for c in q_loads(h_prev, k_prev):
                    c.wait()

            def fetch_q(h=h, pair=pair, j=j):
                if j == 0:
                    q_copy(pair).wait()
                for c in q_loads(h, j):
                    c.start()

            if u == 0:
                pl.when(h >= 1)(fetch_q)
            else:
                fetch_q()

            def tile(t, c, fetch_q=fetch_q, pair=pair, u=u, h=h, j=j, w_now=w_now, w_next=w_next, kv_now=kv_now, kv_prev=kv_prev, k_prev=k_prev, h_prev=h_prev):
                if u == 0:
                    @pl.when((h == 0) & (t == n_batch // 2))
                    def _():
                        for b in range(n_batch):
                            x_remote(b).wait()
                        fetch_q()

                @pl.when(pair + 1 < n_pairs)
                def _():
                    relayout((raw_k, raw_v)[j], w_next, j, t * part, part)

                side = lax.rem(core + t // 2, 2)
                r = pl.ds(pl.multiple_of(lax.rem(t, 2) * big, big), big)
                for sel in range(2):
                    p = weights(h_prev, t, sel, kv_prev, k_prev)
                    kv_now[sel, side, r, :] = jnp.dot(x_buf[side, r, :], w_now[j, sel], preferred_element_type=F32).astype(BF16)
                    weighted(p, t, sel, kv_prev, k_prev)

                @pl.when(h >= 1)
                def _():
                    o_piece(h - 1, k_prev, t).start()

                return c

            lax.fori_loop(0, n_batch, tile, 0)

            @pl.when(pair + 2 < n_pairs)
            def _(j=j, pair=pair):
                raw_copy((wk_hbm, wv_hbm)[j], pair + 2, j).start()

            @pl.when(h >= 1)
            def _():
                s_copy(h - 1, k_prev).start()
                oo_copy(h - 1, k_prev).start()
        return carry

    lax.fori_loop(0, n_heads // 4, four_heads, 0)

    n_wo = wo_hbm.shape[0] // 2
    wo_copies = [pltpu.make_async_copy(wo_hbm.at[pl.ds(i * n_wo, n_wo)], x_buf.at[i], wo_sem.at[i]) for i in range(2)]
    for c in wo_copies:
        c.start()

    final = n_heads - 1
    o_copy(final - 2, 1).wait_send()
    s_copy(final - 2, 1).wait_send()
    oo_copy(final - 2, 1).wait()

    for c in q_loads(final, 1):
        c.wait()

    def last_attention(b, c, side):
        weighted(weights(final, b, side, kv_b, 1), b, side, kv_b, 1)
        if side == 1:
            o_piece(final, 1, b).start()
        return c

    lax.fori_loop(0, n_batch, functools.partial(last_attention, side=1), 0)
    s_copy(final, 1).start()
    lax.fori_loop(0, n_batch, functools.partial(last_attention, side=0), 0)
    oo_copy(final, 1).start()

    half_rows = n_q // 2
    n_half = n_batch // 2

    def c_copies(h, i):
        r = pl.ds(i * half_rows, half_rows)
        return (pltpu.make_async_copy(oown_hbm.at[h, r], o_buf.at[0, 0, r], c_sem.at[0, i]),
                pltpu.make_async_copy(orecv_hbm.at[h, r], c_rx.at[i], c_sem.at[1, i]))

    def att_slot(h):
        hg = head0 + h
        return hg // per_att, pl.ds(pl.multiple_of(lax.rem(hg, per_att) * head_dim, head_dim), head_dim)

    def a_copy(h, k):
        side, lanes = att_slot(h)
        return pltpu.make_async_remote_copy(att_tx.at[k], q_in.at[:, side, :, lanes], a_ssem.at[k], a_rsem.at[h], **to(partner))

    def combine(h, k, following):
        t1, t2 = s_buf[h, 0].T, s_recv[h].T
        m1, l1, m2, l2 = t1[:, 0:1], t1[:, 1:2], t2[:, 0:1], t2[:, 1:2]
        m = jnp.maximum(m1, m2)
        f1, f2 = jnp.exp(m1 - m), jnp.exp(m2 - m)
        den = l1 * f1 + l2 * f2
        f1, f2 = f1 / den, f2 / den
        side, lanes = att_slot(h)
        for i in range(2):
            for c in c_copies(h, i):
                c.wait()
            for b in range(i * n_half, (i + 1) * n_half):
                r = slice(b * half_q, (b + 1) * half_q)
                rc = slice((b - i * n_half) * half_q, (b - i * n_half + 1) * half_q)
                res = (o_buf[0, 0, r, :] * f1[r] + c_rx[i, rc, :] * f2[r]).astype(BF16)
                lo, hi = res[:q_loc], res[q_loc:]
                q_in[b, side, :, lanes] = jnp.where(core == 0, lo, hi)
                att_tx[k, b] = jnp.where(core == 0, hi, lo)
            following(i)

    oo_copy(final - 1, 0).wait()
    o_copy(final - 1, 0).wait_send()
    s_copy(final - 1, 0).wait_send()
    pl.semaphore_wait(free_sem, 1)
    o_copy(0, 0).wait_recv()
    s_copy(0, 0).wait_recv()
    for i in range(2):
        for c in c_copies(0, i):
            c.start()

    def combine_step(h, carry):
        k = lax.rem(h, 2)

        @pl.when(h + 1 < final)
        def _():
            o_copy(h + 1, 0).wait_recv()
            s_copy(h + 1, 0).wait_recv()

        @pl.when(h >= 2)
        def _():
            a_copy(h - 2, k).wait_send()

        def following(i):
            @pl.when(h + 1 < final)
            def _():
                for c in c_copies(h + 1, i):
                    c.start()

        combine(h, k, following)
        a_copy(h, k).start()
        return carry

    lax.fori_loop(0, final, combine_step, 0)
    for c in wo_copies:
        c.wait()
    for h in range(final):
        a_copy(h, 0).wait_recv()

    width = out_buf.shape[2]
    n_out = n_batch * q_loc
    most = final * head_dim
    rest = 2 * n_wo - d_model
    n_cols = d_model // width

    def columns(n):
        return pl.ds(pl.multiple_of(n * width, width), width)

    def early_tile(n, carry):
        cols = columns(n)
        acc = jnp.dot(q_in[:, 0, :, 0:most].reshape(n_out, most), x_buf[0, 0:most, cols], preferred_element_type=F32)
        acc += jnp.dot(q_in[:, 0, :, n_wo:].reshape(n_out, d_model - n_wo), x_buf[1, 0:d_model - n_wo, cols], preferred_element_type=F32)
        acc += jnp.dot(q_in[:, 1, :, 0:rest - head_dim].reshape(n_out, rest - head_dim), x_buf[1, d_model - n_wo:most, cols], preferred_element_type=F32)
        acc_buf[:, cols] = acc
        return carry

    lax.fori_loop(0, n_cols, early_tile, 0)
    k = final % 2
    oo_copy(final, 1).wait()
    o_copy(final, 1).wait_send()
    s_copy(final, 1).wait_send()
    a_copy(final - 2, k).wait_send()
    o_copy(final, 1).wait_recv()
    s_copy(final, 1).wait_recv()
    for i in range(2):
        for c in c_copies(final, i):
            c.start()
    combine(final, k, lambda i: None)
    a_copy(final, k).start()
    a_copy(final - 1, 1 - k).wait_send()
    a_copy(final, k).wait_send()
    a_copy(final, k).wait_recv()

    def out_copy(n, k):
        return pltpu.make_async_copy(out_buf.at[k], out_hbm.at[:, columns(n)], out_sem.at[k])

    def out_tile(n, carry):
        k = lax.rem(n, 2)

        @pl.when(n >= 2)
        def _():
            out_copy(n - 2, k).wait()

        cols = columns(n)
        acc = acc_buf[:, cols] + jnp.dot(q_in[:, 0, :, most:n_wo].reshape(n_out, head_dim), x_buf[0, most:n_wo, cols], preferred_element_type=F32)
        acc += jnp.dot(q_in[:, 1, :, rest - head_dim:rest].reshape(n_out, head_dim), x_buf[1, most:n_wo, cols], preferred_element_type=F32)
        out_buf[k] = acc.astype(BF16)
        out_copy(n, k).start()
        return carry

    lax.fori_loop(0, n_cols, out_tile, 0)
    for n in (n_cols - 2, n_cols - 1):
        out_copy(n, n % 2).wait()


def solution(mesh):
    def local_step(query_in, memory, mem_len, w_query, w_key, w_value, w_out):
        n_batch, q_loc, d_model = query_in.shape
        mem_local = memory.shape[1]
        head_dim = w_query.shape[2]
        n_heads = w_query.shape[1] // 2
        n_pairs = n_heads // 2
        n_q = n_batch * 2 * q_loc
        out_width = 512
        any_spec = pl.BlockSpec(memory_space=pl.ANY)
        part = jax.ShapeDtypeStruct((n_heads, n_q, head_dim), F32)
        dma = pltpu.SemaphoreType.DMA
        q_part = jax.ShapeDtypeStruct((n_heads, n_q, head_dim), BF16)
        out = pl.pallas_call(
            attend_kernel,
            out_shape=(jax.ShapeDtypeStruct((n_batch * q_loc, d_model), BF16), part, part, q_part, q_part),
            in_specs=[pl.BlockSpec(memory_space=pltpu.SMEM)] + [any_spec] * 6,
            out_specs=(any_spec,) * 5,
            scratch_shapes=[
                pltpu.VMEM((2, n_batch * mem_local, d_model), BF16),
                pltpu.VMEM((n_batch, 2, q_loc, d_model), BF16),
                pltpu.VMEM((2, 2, n_q, head_dim), BF16),
                pltpu.VMEM((d_model, 2, head_dim), BF16),
                pltpu.VMEM((d_model, 2, head_dim), BF16),
                pltpu.VMEM((2, 2, d_model, head_dim), BF16),
                pltpu.VMEM((2, 2, d_model, head_dim), BF16),
                pltpu.VMEM((2, 2, n_batch * mem_local, head_dim), BF16),
                pltpu.VMEM((2, 2, n_batch * mem_local, head_dim), BF16),
                pltpu.VMEM((2, 2, n_q, head_dim), F32),
                pltpu.VMEM((n_heads, 2, 8, n_q), F32),
                pltpu.VMEM((n_heads, 8, n_q), F32),
                pltpu.VMEM((2, n_q // 2, head_dim), F32),
                pltpu.VMEM((2, n_batch, q_loc, head_dim), BF16),
                pltpu.VMEM((2, n_batch * q_loc, out_width), BF16),
                pltpu.VMEM((n_batch * q_loc, d_model), F32),
                dma((n_batch,)), dma((n_batch,)), dma((n_batch,)), dma, dma, dma, dma((2,)),
                dma((n_pairs,)), dma((n_pairs,)), dma((2, 2)), dma((2,)), dma((n_heads,)), dma((2,)), dma((n_heads,)), dma((2,)),
                dma((2,)), dma((2, 2)), dma((2,)), dma((n_heads,)), dma((2,)), pltpu.SemaphoreType.REGULAR,
            ],
            compiler_params=pltpu.CompilerParams(collective_id=0, has_side_effects=True, vmem_limit_bytes=67043328),
        )(mem_len, query_in, memory, w_query, w_key, w_value, w_out.reshape(2 * n_heads * head_dim, d_model))[0]
        return out.reshape(n_batch, q_loc, d_model)

    return jax.shard_map(local_step, mesh=mesh, in_specs=(P('replica', 'seq', None), P('replica', 'seq', None), P('replica'), P(), P(), P(), P()), out_specs=P('replica', 'seq', None), check_vma=False)
```
